16 devices in a mesh: rep: 4 (over y, z, core), dp: 4 (over x).
Axes of the slice: x: 4, y: 2, z: 1, core: 2. Of those that a mesh axis runs over, the one named last changes fastest.
The devices are a block of a 4x4x8 slice.
Arguments:
- a: bfloat16 [16, 4, 8192, 512], P(('rep', 'dp')), parts along dimension 0
- g: bfloat16 [16, 4, 8192, 1280], P(('rep', 'dp')), parts along dimension 0
Outputs:
- output: bfloat16 [16, 512, 1280], P('rep'), parts along dimension 0
There are 4 independent parts. The reference program is written for one: setup_inputs(seed, part) draws one part's arguments, and reference() takes and returns one part's arrays. A program takes and returns all parts, laid end to end along the dimension named above; each array names one.
All inputs are finite; a program needn't handle non-finite values.
Results may differ from the reference program's by a relative error of at most 0.012.
Values are sent between devices in bfloat16 or wider.
A program may use at most 768 MiB of HBM per device.

```python
import jax
import jax.numpy as jnp
from jax import lax

DEVICES = 4
MATRICES = 4
TOKENS = 8192
D = 512
FF = 1280


def setup_inputs(seed: int = 0, part: int = 0) -> dict:
    ka, kg, ks = (jax.random.fold_in(k, part) for k in jax.random.split(jax.random.key(seed), 3))
    size = 2.0 ** jax.random.uniform(ks, (DEVICES, MATRICES, 1, 1), jnp.float32, -1.0, 1.0)
    a = jax.random.normal(ka, (DEVICES, MATRICES, TOKENS, D), jnp.float32)
    g = size * jax.random.normal(kg, (DEVICES, MATRICES, TOKENS, FF), jnp.float32) * (DEVICES * TOKENS) ** -0.5
    return {"a": a.astype(jnp.bfloat16), "g": g.astype(jnp.bfloat16)}


def reference(a, g):
    def take(so_far, one):
        return so_far + jnp.einsum("ntd,ntf->ndf", *one, preferred_element_type=jnp.float32), None

    return lax.scan(take, jnp.zeros((MATRICES, D, FF), jnp.float32), (a, g))[0].astype(jnp.bfloat16)
```

```python
import functools

import jax
import jax.numpy as jnp
from jax import lax
from jax.experimental import pallas as pl
from jax.experimental.pallas import tpu as pltpu
from jax.sharding import PartitionSpec as P

C = 256
KF = 1
GS = 3
LF, LO = 2, 4
AG_EVERY = 2
MESH = pl.DeviceIdType.MESH
F32, BF16 = jnp.float32, jnp.bfloat16


def kernel(ring, a_hbm, g_hbm, o_ref, abuf, gbuf, acc, far_s, mid_s, leaf_s, far_r, mid_r, leaf_r,
           a_sem, g_sem, ss, rs):
    mats, tokens, d = a_hbm.shape
    cols = g_hbm.shape[2] // C
    units = mats * cols
    rows = d // ring
    kt = tokens // KF
    me = lax.axis_index("dp")

    def at(x):
        return lax.rem(me + x + 2 * ring, ring)

    def a_copy(n, k):
        t = pl.ds(k * kt, kt)
        return pltpu.make_async_copy(a_hbm.at[n, t], abuf.at[lax.rem(n, 2), t], a_sem.at[lax.rem(n, 2), k])

    def g_copy(u, k):
        n, j = lax.div(u, cols), lax.rem(u, cols)
        t = pl.ds(k * kt, kt)
        return pltpu.make_async_copy(
            g_hbm.at[n, t, pl.ds(pl.multiple_of(j * C, C), C)], gbuf.at[lax.rem(u, GS), t], g_sem.at[lax.rem(u, GS), k])

    def i32(x):
        return jnp.int32(x)

    for k in range(KF):
        a_copy(i32(0), k).start()
        g_copy(i32(0), k).start()
    for k in range(KF):
        g_copy(i32(1), k).start()

    barrier = pltpu.get_barrier_semaphore()
    for x in (1, -1):
        pl.semaphore_signal(barrier, inc=1, device_id={"dp": at(x)}, device_id_type=MESH)
    pl.semaphore_wait(barrier, 2)

    def sign(u):
        return 1 - 2 * lax.rem(u, 2)

    def block(u, r):
        return o_ref.at[lax.div(u, cols), pl.ds(pl.multiple_of(r * rows, rows), rows),
                        pl.ds(pl.multiple_of(lax.rem(u, cols) * C, C), C)]

    def far(u):
        return pltpu.make_async_remote_copy(far_s.at[u], far_r.at[u], ss.at[0, u], rs.at[0, u],
                                            device_id={"dp": at(sign(u))}, device_id_type=MESH)

    def leaf(u):
        return pltpu.make_async_remote_copy(leaf_s.at[u], leaf_r.at[u], ss.at[1, u], rs.at[1, u],
                                            device_id={"dp": at(-sign(u))}, device_id_type=MESH)

    def mid(u):
        return pltpu.make_async_remote_copy(mid_s.at[u], mid_r.at[u], ss.at[2, u], rs.at[2, u],
                                            device_id={"dp": at(sign(u))}, device_id_type=MESH)

    def gather(u, i, owner, x):
        b = block(u, owner)
        return pltpu.make_async_remote_copy(b, b, ss.at[3 + i, u], rs.at[3 + i, u],
                                            device_id={"dp": at(x)}, device_id_type=MESH)

    def term(u, r):
        return acc[lax.rem(u, LO + 1), pl.ds(pl.multiple_of(r * rows, rows), rows)]

    def do_raw(u):
        s = sign(u)
        far_s[u] = term(u, at(2)).astype(BF16)
        far(u).start()
        leaf_s[u] = term(u, at(-s)).astype(BF16)
        leaf(u).start()

    def do_mid(u):
        far(u).wait_recv()
        mid_s[u] = (term(u, at(sign(u))) + far_r[u].astype(F32)).astype(BF16)
        mid(u).start()

    def do_own(u):
        leaf(u).wait_recv()
        mid(u).wait_recv()
        block(u, me)[...] = (term(u, me) + mid_r[u].astype(F32) + leaf_r[u].astype(F32)).astype(BF16)

    def do_gather(u):
        s = sign(u)
        gather(u, 0, me, -s).start()
        gather(u, 1, me, s).start()

    def do_pass(u):
        s = sign(u)
        gather(u, 0, at(s), -s).wait_recv()
        gather(u, 2, at(s), -s).start()

    def done(u):
        s = sign(u)
        gather(u, 1, at(-s), s).wait_recv()
        gather(u, 2, at(2), -s).wait_recv()
        far(u).wait_send()
        leaf(u).wait_send()
        mid(u).wait_send()
        for i in range(3):
            gather(u, i, me, s).wait_send()

    wait = -(-LO // AG_EVERY)
    dims = (((0,), (0,)), ((), ()))

    def slot(u, carry):
        n, j = lax.div(u, cols), lax.rem(u, cols)

        @pl.when(u + 2 < units)
        def _():
            for k in range(KF):
                g_copy(u + 2, k).start()

        @pl.when((j < KF) & (n + 1 < mats))
        def _():
            a_copy(n + 1, j).start()

        sl, gl, cl = lax.rem(n, 2), lax.rem(u, GS), lax.rem(u, LO + 1)
        for k in range(KF):
            g_copy(u, k).wait()

            @pl.when(j == 0)
            def _():
                a_copy(n, k).wait()
            t = pl.ds(k * kt, kt)
            p = lax.dot_general(abuf[sl, t], gbuf[gl, t], dims, preferred_element_type=F32)
            if k:
                acc[cl] += p
            else:
                acc[cl] = p
        do_raw(u)

        @pl.when(u >= LF)
        def _():
            do_mid(u - LF)

        @pl.when(u >= LO)
        def _():
            do_own(u - LO)

        @pl.when((lax.rem(u, AG_EVERY) == 0) & (u >= wait * AG_EVERY))
        def _():
            do_gather(lax.div(u, AG_EVERY) - wait)
        return carry

    lax.fori_loop(0, units, slot, 0)
    sent = (units - 1) // AG_EVERY - wait + 1
    c = lambda f: (lambda u, _: (f(u), _)[1])
    lax.fori_loop(units - LF, units, c(do_mid), 0)
    lax.fori_loop(sent, sent + 4, c(do_gather), 0)
    lax.fori_loop(units - LO, units, c(do_own), 0)
    lax.fori_loop(sent + 4, units, c(do_gather), 0)
    lax.fori_loop(0, units, c(do_pass), 0)
    lax.fori_loop(0, units, c(done), 0)


def solution(mesh):
    ring = mesh.shape["dp"]

    def body(a, g):
        _, mats, tokens, d = a.shape
        ff = g.shape[-1]
        units, rows = mats * (ff // C), d // ring
        blk = pltpu.VMEM((units, rows, C), BF16)
        return pl.pallas_call(
            functools.partial(kernel, ring),
            out_shape=pltpu.VMEM((mats, d, ff), BF16),
            in_specs=[pl.BlockSpec(memory_space=pl.ANY)] * 2,
            out_specs=pl.BlockSpec(memory_space=pltpu.VMEM),
            scratch_shapes=[
                pltpu.VMEM((2, tokens, d), BF16),
                pltpu.VMEM((GS, tokens, C), BF16),
                pltpu.VMEM((LO + 1, d, C), F32),
                blk, blk, blk, blk, blk, blk,
                pltpu.SemaphoreType.DMA((2, KF)),
                pltpu.SemaphoreType.DMA((GS, KF)),
                pltpu.SemaphoreType.DMA((6, units)),
                pltpu.SemaphoreType.DMA((6, units)),
            ],
            compiler_params=pltpu.CompilerParams(
                collective_id=0, has_side_effects=True, vmem_limit_bytes=46 << 20),
            cost_estimate=pl.CostEstimate(
                flops=2 * mats * tokens * d * ff, bytes_accessed=2 * mats * tokens * (d + ff), transcendentals=0),
        )(a[0], g[0])

    return jax.shard_map(body, mesh=mesh, in_specs=P(("rep", "dp")), out_specs=P("rep"), check_vma=False)
```

```python
import functools

import jax
import jax.numpy as jnp
from jax import lax
from jax.experimental import pallas as pl
from jax.experimental.pallas import tpu as pltpu
from jax.sharding import PartitionSpec as P

C = 256
LEAD = 2
AHEAD = 2
GS = LEAD + AHEAD + 1
LO = 2
AG_EVERY = 2
AG_HEAD = 4
KS = 1
MESH = pl.DeviceIdType.MESH
F32, BF16 = jnp.float32, jnp.bfloat16
DIMS = (((0,), (0,)), ((), ()))


def kernel(ring, a_hbm, g_hbm, o_ref, abuf, gbuf, own, far_s, mid_s, leaf_s, far_r, mid_r, leaf_r,
           part, a_sem, g_sem, k_sem, ss, rs):
    mats, tokens, d = a_hbm.shape
    cols = g_hbm.shape[2] // C
    units = mats * cols
    rows = d // ring
    me = lax.axis_index("dp")

    def at(x):
        return lax.rem(me + x + ring, ring)

    def col(r, width):
        return pl.ds(pl.multiple_of(r * width, width), width)

    def a_copy(n, x):
        sl = lax.rem(n, 2)
        return pltpu.make_async_copy(a_hbm.at[n, :, col(at(x), rows)], abuf.at[sl, x], a_sem.at[sl, x])

    def g_copy(u):
        sl = lax.rem(u, GS)
        return pltpu.make_async_copy(g_hbm.at[lax.div(u, cols), :, col(lax.rem(u, cols), C)], gbuf.at[sl], g_sem.at[sl])

    def i32(x):
        return jnp.int32(x)

    def piece(i, k):
        t = pl.ds(k * (tokens // KS), tokens // KS)
        if i == 2:
            return pltpu.make_async_copy(g_hbm.at[0, t, pl.ds(0, C)], gbuf.at[0, t], k_sem.at[2, k])
        x = 2 + i
        return pltpu.make_async_copy(a_hbm.at[0, t, col(at(x), rows)], abuf.at[0, x, t], k_sem.at[i, k])

    for k in range(KS):
        for i in range(3):
            piece(i, k).start()
    a_copy(i32(0), 1).start()
    for u in range(1, AHEAD + 1):
        g_copy(i32(u)).start()
    a_copy(i32(0), 0).start()

    barrier = pltpu.get_barrier_semaphore()
    for x in (1, -1):
        pl.semaphore_signal(barrier, inc=1, device_id={"dp": at(x)}, device_id_type=MESH)

    def remote(src, dst, i, u, x):
        return pltpu.make_async_remote_copy(src, dst, ss.at[i, u], rs.at[i, u], device_id={"dp": at(x)}, device_id_type=MESH)

    def block(u, r):
        return o_ref.at[lax.div(u, cols), col(r, rows), col(lax.rem(u, cols), C)]

    def far(u, s):
        return remote(far_s.at[u], far_r.at[u], 0, u, s)

    def leaf(u, s):
        return remote(leaf_s.at[u], leaf_r.at[u], 1, u, -s)

    def mid(u, s):
        return remote(mid_s.at[u], mid_r.at[u], 2, u, s)

    def gather(u, i, owner, x):
        return remote(block(u, owner), block(u, owner), 3 + i, u, x)

    def sign(u):
        return 1 - 2 * lax.rem(u, 2)

    def beside(s):
        return lax.rem(ring - s, ring)

    def terms(u, x, y):
        sl = lax.rem(lax.div(u, cols), 2)
        lhs = jnp.concatenate([abuf[sl, x], abuf[sl, y]], axis=1)
        return lax.dot_general(lhs, gbuf[lax.rem(u, GS)], DIMS, preferred_element_type=F32)

    def send(u, s, p):
        far_s[u] = p[:rows].astype(BF16)
        far(u, s).start()
        leaf_s[u] = p[rows:].astype(BF16)
        leaf(u, s).start()

    def first(u):
        n, j, s = lax.div(u, cols), lax.rem(u, cols), sign(u)

        @pl.when(u + AHEAD < units)
        def _():
            g_copy(u + AHEAD).start()

        @pl.when((j == LEAD) & (n + 1 < mats))
        def _():
            a_copy(n + 1, 2).start()
            a_copy(n + 1, 3).start()

        @pl.when((j == LEAD + 1) & (n + 1 < mats))
        def _():
            a_copy(n + 1, 1).start()
            a_copy(n + 1, 0).start()

        @pl.when((j == 0) & (n > 0))
        def _():
            a_copy(n, 2).wait()
            a_copy(n, 3).wait()
            a_copy(n, 1).wait()

        @pl.when(u == 1)
        def _():
            a_copy(n, 1).wait()

        g_copy(u).wait()
        send(u, s, terms(u, 2, beside(s)))

    def second(u):
        s = sign(u)

        @pl.when(lax.rem(u, cols) == 0)
        def _():
            a_copy(lax.div(u, cols), 0).wait()

        p = terms(u, beside(-s), 0)
        own[lax.rem(u, LO + 1)] = p[rows:]
        far(u, s).wait_recv()
        mid_s[u] = (p[:rows] + far_r[u].astype(F32)).astype(BF16)
        mid(u, s).start()

    def finish(u):
        leaf(u, sign(u)).wait_recv()
        mid(u, sign(u)).wait_recv()
        block(u, me)[...] = (own[lax.rem(u, LO + 1)] + mid_r[u].astype(F32) + leaf_r[u].astype(F32)).astype(BF16)

    def spread(u):
        gather(u, 0, me, -sign(u)).start()
        gather(u, 1, me, sign(u)).start()

    def hand_on(u):
        s = sign(u)
        gather(u, 0, at(s), -s).wait_recv()
        gather(u, 2, at(s), -s).start()

    def done(u):
        s = sign(u)
        gather(u, 1, at(-s), s).wait_recv()
        gather(u, 2, at(2), -s).wait_recv()
        far(u, s).wait_send()
        leaf(u, s).wait_send()
        mid(u, s).wait_send()
        for i in range(3):
            gather(u, i, me, s).wait_send()

    wait = -(-LO // AG_EVERY)

    for k in range(KS):
        for i in range(3):
            piece(i, k).wait()
        t = pl.ds(k * (tokens // KS), tokens // KS)
        lhs = jnp.concatenate([abuf[0, 2, t], abuf[0, 3, t]], axis=1)
        p = lax.dot_general(lhs, gbuf[0, t], DIMS, preferred_element_type=F32)
        if k == 0:
            part[...] = p
        elif k < KS - 1:
            part[...] += p
    pl.semaphore_wait(barrier, 2)
    send(i32(0), 1, p)

    def step(u, carry):
        v = u - LEAD

        @pl.when(u < units)
        def _():
            first(u)

        @pl.when(v >= 0)
        def _():
            second(v)

        @pl.when(v >= LO)
        def _():
            finish(v - LO)

        @pl.when((lax.rem(v, AG_EVERY) == 0) & (v >= wait * AG_EVERY))
        def _():
            spread(lax.div(v, AG_EVERY) - wait)
        return carry

    lax.fori_loop(1, units + LEAD, step, 0)
    sent = (units - 1) // AG_EVERY - wait + 1

    def each(f, lo, hi):
        def body(u, carry):
            f(u)
            return carry
        lax.fori_loop(lo, hi, body, 0)

    each(spread, sent, sent + AG_HEAD)
    each(finish, units - LO, units)
    each(spread, sent + AG_HEAD, units)
    each(hand_on, 0, units)
    each(done, 0, units)


def solution(mesh):
    ring = mesh.shape["dp"]

    def body(a, g):
        _, mats, tokens, d = a.shape
        ff = g.shape[-1]
        units, rows = mats * (ff // C), d // ring
        blk = pltpu.VMEM((units, rows, C), BF16)
        return pl.pallas_call(
            functools.partial(kernel, ring),
            out_shape=pltpu.VMEM((mats, d, ff), BF16),
            in_specs=[pl.BlockSpec(memory_space=pl.ANY)] * 2,
            out_specs=pl.BlockSpec(memory_space=pltpu.VMEM),
            scratch_shapes=[
                pltpu.VMEM((2, ring, tokens, rows), BF16),
                pltpu.VMEM((GS, tokens, C), BF16),
                pltpu.VMEM((LO + 1, rows, C), F32),
                blk, blk, blk, blk, blk, blk,
                pltpu.VMEM((2 * rows, C), F32),
                pltpu.SemaphoreType.DMA((2, ring)),
                pltpu.SemaphoreType.DMA((GS,)),
                pltpu.SemaphoreType.DMA((3, KS)),
                pltpu.SemaphoreType.DMA((6, units)),
                pltpu.SemaphoreType.DMA((6, units)),
            ],
            compiler_params=pltpu.CompilerParams(
                collective_id=0, has_side_effects=True, vmem_limit_bytes=50 << 20),
            cost_estimate=pl.CostEstimate(
                flops=2 * mats * tokens * d * ff, bytes_accessed=2 * mats * tokens * (d + ff), transcendentals=0),
        )(a[0], g[0])

    return jax.shard_map(body, mesh=mesh, in_specs=P(("rep", "dp")), out_specs=P("rep"), check_vma=False)
```
